32 devices in a mesh: rows: 4 (over y, x), cols: 8 (over z, core).
Axes of the slice: x: 2, y: 2, z: 4, core: 2. Of those that a mesh axis runs over, the one named last changes fastest.
Arguments:
- factor_u: float32 [4, 2048, 128], P('rows', 'cols'), may hold values from -2 to 2
- factor_v: float32 [8, 512, 128], P('cols', 'rows'), may hold values from -2 to 2
- values: bfloat16 [4, 8, 8, 256, 256], P('rows', 'cols'), may hold values from -6 to 6
- mask_words: int32 [4, 8, 8, 16, 256], P('rows', 'cols'), may hold values from 0 to 65535, as said below
- tile_cols: int32 [4, 8, 8], P('rows', 'cols'), may hold values from 0 to 1
Outputs:
- new_u: float32 [4, 2048, 128], P('rows', 'cols')
- new_v: float32 [8, 512, 128], P('cols', 'rows')
- loss: float32 [], replicated
The draws below stay inside these ranges and needn't reach their ends.
Inputs may be any that keep to these rules, and one draw needn't show every extreme that they name: `mask_words`: bit b of word w of a slot marks the entry in row 16 w + b of the tile.
All inputs are finite; a program needn't handle non-finite values.
Results may differ from the reference program's by a relative error of at most 0.02.
Values may be sent and summed in bfloat16 or wider, within the bound.
No kernel may reach another device: no remote copies, remote signals or barrier semaphores. Data moves between devices by JAX's collectives and lax.ppermute only.
A program may use at most 64 MiB of HBM per device.

```python
import jax
import jax.numpy as jnp
from jax import lax

K = 128
TILE = 256
BAND_U = 2048
BAND_V = 512
ROW_TILES = 8
COL_TILES = 2
ENTRIES = 16777216
N_ROWS = 4
N_COLS = 8


def draw_mask_words(key, part):
    level_key = jax.random.fold_in(key, 11)
    ceiling_key = jax.random.fold_in(key, 12)
    bit_key = jax.random.fold_in(key, 13)
    levels = jax.random.randint(level_key, (N_ROWS, N_COLS, ROW_TILES), 0, 9)
    ceiling = jax.random.randint(ceiling_key, (N_ROWS, N_COLS, 1), 3, 10)
    levels = jnp.minimum(levels, ceiling)
    shifts = jnp.arange(16, dtype=jnp.int32)

    def draw_row(row_index):
        samples = jax.random.randint(jax.random.fold_in(bit_key, row_index), (N_COLS, ROW_TILES, TILE // 16, 16, TILE), 0, 8)
        bit_values = (samples < levels[row_index][:, :, None, None, None]).astype(jnp.int32)
        packed = jnp.sum(jnp.left_shift(bit_values, shifts[:, None]), axis=3)
        return packed.astype(jnp.int32)
    return lax.map(draw_row, jnp.arange(N_ROWS, dtype=jnp.int32))


def touch_ends(array, stream_key, least, top_value):
    dims = array.shape
    index_at = [jax.random.randint(jax.random.fold_in(stream_key, axis), (), 0, dims[axis]) for axis in range(len(dims))]
    array = array.at[tuple(index_at)].set(least)
    longest = dims.index(max(dims))
    index_at[longest] = (index_at[longest] + 1) % dims[longest]
    return array.at[tuple(index_at)].set(top_value)


def steps_of(key, shape, split, low, high):
    def one(dim, blocks):
        draws = jax.random.uniform(jax.random.fold_in(jax.random.fold_in(key, 6), dim), (blocks,), jnp.float32, low / len(split), high / len(split))
        return jnp.repeat(jnp.exp(draws), shape[dim] // blocks).reshape((-1,) + (1,) * (len(shape) - dim - 1))

    gain = one(*split[0])
    for cut in split[1:]:
        gain = gain * one(*cut)
    return gain


def gaussian(rng, shape, scale, bound, pieces=(), kind=jnp.bfloat16):
    result = scale * jax.random.normal(rng, shape, jnp.float32)
    if pieces:
        result = result * steps_of(rng, shape, pieces, -0.22, 0.18)
    return jnp.clip(result, -bound, bound).astype(kind)


def setup_inputs(seed: int = 0) -> dict:
    splits = jax.random.split(jax.random.key(seed), 6)
    return {
        "factor_u": gaussian(splits[0], (N_ROWS, BAND_U, K), 0.3, 2.0, ((0, 4), (1, 8)), jnp.float32),
        "factor_v": gaussian(splits[1], (N_COLS, BAND_V, K), 0.3, 2.0, ((0, 8), (1, 4)), jnp.float32),
        "values": gaussian(splits[2], (N_ROWS, N_COLS, ROW_TILES, TILE, TILE), 1.0, 6.0, ((0, 4), (1, 8))),
        "mask_words": draw_mask_words(jax.random.fold_in(splits[5], 71), 0),
        "tile_cols": touch_ends(jax.random.randint(splits[4], (N_ROWS, N_COLS, ROW_TILES), 0, COL_TILES), jax.random.fold_in(splits[4], 1), 0, COL_TILES - 1).astype(jnp.int32),
    }


step_rate = 0.01
ridge_weight = 0.1


def decode(mask_bits):
    shifts = jnp.arange(16, dtype=jnp.int32)
    bit_values = jnp.bitwise_and(jnp.right_shift(mask_bits[..., None, :], shifts[:, None]), 1)
    lead = mask_bits.shape[:-2]
    return bit_values.reshape(lead + (mask_bits.shape[-2] * 16, mask_bits.shape[-1])).astype(jnp.float32)


def rounded(array_in):
    return lax.optimization_barrier(array_in.astype(jnp.bfloat16)).astype(jnp.float32)


def device_terms(left_band, right_band, tile_values, mask_bits, column_ids):
    left_rows = left_band.reshape(-1, TILE, K).astype(jnp.float32)
    right_tiles = right_band.reshape(-1, TILE, K)
    right_rows = jnp.take(right_tiles, column_ids, axis=0).astype(jnp.float32)
    observed = decode(mask_bits)
    predicted = jnp.einsum("sik,sjk->sij", left_rows, right_rows, precision=lax.Precision.HIGHEST)
    residual = observed * (predicted - tile_values.astype(jnp.float32))
    resid_low = rounded(residual)
    grad_rows = jnp.einsum("sij,sjk->sik", resid_low, right_rows, precision=lax.Precision.HIGHEST)
    grad_cols = jnp.einsum("sij,sik->sjk", resid_low, left_rows, precision=lax.Precision.HIGHEST)
    col_sums = jax.ops.segment_sum(grad_cols, column_ids, num_segments=COL_TILES)
    squares = 0.5 * jnp.sum(residual * residual)
    return grad_rows.reshape(-1, K), col_sums.reshape(-1, K), squares


def reference(factor_u, factor_v, values, mask_words, tile_cols):
    u_low = factor_u.astype(jnp.bfloat16)
    v_low = factor_v.astype(jnp.bfloat16)

    def row_group(running, row_index):
        v_total, data_total = running

        def col_group(u_sum, col_index):
            grad_rows, col_sums, squares = device_terms(
                u_low[row_index], v_low[col_index], values[row_index, col_index],
                mask_words[row_index, col_index], tile_cols[row_index, col_index])
            return u_sum + rounded(grad_rows), (rounded(col_sums), squares)

        u_sum, outputs = lax.scan(col_group, jnp.zeros((BAND_U, K), jnp.float32),
                                  jnp.arange(N_COLS, dtype=jnp.int32))
        col_parts, square_parts = outputs
        return (v_total + col_parts, data_total + jnp.sum(square_parts)), u_sum

    initial = (jnp.zeros((N_COLS, BAND_V, K), jnp.float32), jnp.zeros((), jnp.float32))
    finals, grad_u = lax.scan(row_group, initial, jnp.arange(N_ROWS, dtype=jnp.int32))
    grad_v, data_total = finals
    penalty = 0.5 * ridge_weight * (jnp.sum(factor_u * factor_u) + jnp.sum(factor_v * factor_v))
    loss = (data_total + penalty) / ENTRIES
    new_u = factor_u - step_rate * (grad_u + ridge_weight * factor_u)
    new_v = factor_v - step_rate * (grad_v + ridge_weight * factor_v)
    return new_u, new_v, loss
```

```python
import functools

import jax
import jax.numpy as jnp
from jax import lax
from jax.experimental import pallas as pl
from jax.experimental.pallas import tpu as pltpu
from jax.sharding import PartitionSpec as P


step_rate = 0.01
ridge_weight = 0.1
bf16 = jnp.bfloat16
f32 = jnp.float32
LOSS_ROWS = 16
WORD_BITS = 16


def partners(size, bit):
    return [(i, i ^ bit) for i in range(size)]


def split3(x):
    hi = x.astype(bf16)
    rest = x - hi.astype(f32)
    mid = rest.astype(bf16)
    lo = (rest - mid.astype(f32)).astype(bf16)
    return hi, mid, lo


def vmem_call(body, out_shape, scratch_shapes=(), smem_args=0, n_args=0, **kw):
    specs = [pl.BlockSpec(memory_space=pltpu.SMEM)] * smem_args
    specs += [pl.BlockSpec(memory_space=pltpu.VMEM)] * (n_args - smem_args)
    return pl.pallas_call(
        body,
        out_shape=out_shape,
        in_specs=specs,
        out_specs=jax.tree.map(lambda _: pl.BlockSpec(memory_space=pltpu.VMEM), out_shape),
        scratch_shapes=scratch_shapes,
        **kw,
    )


def tile_kernel(n_cols, n_rows, tile, *refs):
    column_ids, values, words, own_u, own_v = refs[:5]
    u_blocks = refs[5 : 5 + n_cols]
    v_blocks = refs[5 + n_cols : 5 + n_cols + n_rows]
    same, cross, pv_out = refs[5 + n_cols + n_rows : 8 + n_cols + n_rows]
    v_band, v_total = refs[8 + n_cols + n_rows :]
    col = lax.axis_index("cols")
    row = lax.axis_index("rows")
    v_rows = v_blocks[0].shape[0]
    for q in range(n_rows):
        v_band[pl.ds((row ^ q) * v_rows, v_rows), :] = v_blocks[q][...]
    v_total[...] = jnp.zeros_like(v_total)
    block_rows = u_blocks[0].shape[0]
    bit = jnp.left_shift(1, lax.broadcasted_iota(jnp.int32, (WORD_BITS, tile), 0))
    squares = jnp.zeros((8, tile), f32)
    tiles = block_rows // tile
    for q in range(n_cols):
        target = cross if q & 1 else same
        for t in range(tiles):
            slot = (col ^ q) * tiles + t
            start = column_ids[slot] * tile
            left = u_blocks[q][t * tile : (t + 1) * tile, :]
            right = v_band[pl.ds(start, tile), :]
            predicted = lax.dot_general(
                left, right, (((1,), (1,)), ((), ())), preferred_element_type=f32
            )
            diff = predicted - values[slot].astype(f32)
            parts = []
            for w in range(tile // WORD_BITS):
                marks = jnp.broadcast_to(words[slot, w : w + 1, :], (WORD_BITS, tile))
                seen = jnp.bitwise_and(marks, bit) != 0
                parts.append(jnp.where(seen, diff[w * WORD_BITS : (w + 1) * WORD_BITS, :], 0.0))
            residual = jnp.concatenate(parts, axis=0)
            squares += jnp.sum((residual * residual).reshape(-1, 8, tile), axis=0)
            low = residual.astype(bf16)
            grad_rows = jnp.dot(low, right, preferred_element_type=f32)
            target[q // 2, t * tile : (t + 1) * tile, :] = grad_rows.astype(bf16)
            v_total[pl.ds(start, tile), :] += lax.dot_general(
                low, left, (((0,), (0,)), ((), ())), preferred_element_type=f32
            )
    u_own = own_u[...]
    v_own = own_v[...]
    loss = 0.5 * jnp.sum(squares) + 0.5 * ridge_weight * (
        jnp.sum(u_own * u_own) + jnp.sum(v_own * v_own)
    )
    loss_row = jnp.full((1, pv_out.shape[-1]), loss, f32)
    hi, mid, lo = (p.astype(f32) for p in split3(loss_row))
    which = lax.broadcasted_iota(jnp.int32, (LOSS_ROWS, pv_out.shape[-1]), 0)
    packed = jnp.where(which == 0, hi, jnp.where(which == 1, mid, jnp.where(which == 2, lo, 0.0)))
    for q in range(n_rows):
        pv_out[q, :v_rows, :] = v_total[pl.ds((row ^ q) * v_rows, v_rows), :].astype(bf16)
        pv_out[q, v_rows:, :] = packed.astype(bf16)


def pair_kernel(same, got, *outs):
    for q, out in enumerate(outs):
        out[...] = (same[q].astype(f32) + got[q].astype(f32)).astype(bf16)


def v_kernel(n_rows, own_v, pv, *refs):
    got, (new_v, loss_out) = refs[: n_rows - 1], refs[n_rows - 1 :]
    v_rows = own_v.shape[0]
    total = pv[0].astype(f32)
    for block in got:
        total += block[...].astype(f32)
    own = own_v[...]
    new_v[...] = own - step_rate * (total[:v_rows] + ridge_weight * own)
    loss = total[v_rows : v_rows + 1] + total[v_rows + 1 : v_rows + 2] + total[v_rows + 2 : v_rows + 3]
    loss_out[...] = jnp.broadcast_to(loss, loss_out.shape)


def u_kernel(n_pairs, entries, own_u, *refs):
    blocks = refs[:n_pairs]
    losses = refs[n_pairs : 2 * n_pairs]
    new_u, loss_out = refs[2 * n_pairs :]
    total = blocks[0][...].astype(f32)
    for block in blocks[1:]:
        total += block[...].astype(f32)
    own = own_u[...]
    new_u[...] = own - step_rate * (total + ridge_weight * own)
    loss = losses[0][...]
    for other in losses[1:]:
        loss += other[...]
    loss_out[...] = loss * (1.0 / entries)


def per_device(factor_u, factor_v, values, mask_words, tile_cols):
    own_u = factor_u[0]
    own_v = factor_v[0]
    tile_values = values[0, 0]
    words = mask_words[0, 0]
    column_ids = tile_cols[0, 0]
    slots, tile = tile_values.shape[0], tile_values.shape[-1]
    rank = own_u.shape[-1]
    n_rows, n_cols = lax.axis_size("rows"), lax.axis_size("cols")
    block_rows, v_rows = own_u.shape[0], own_v.shape[0]
    far = sorted(range(2, n_cols, 2), reverse=True)

    def send_cols(x, bit):
        return lax.ppermute(x, "cols", partners(n_cols, bit))

    def send_rows(x, bit):
        return lax.ppermute(x, "rows", partners(n_rows, bit))

    u_low = own_u.astype(bf16)
    v_low = own_v.astype(bf16)
    u_blocks = {0: u_low}
    v_blocks = {0: v_low}
    for q in far:
        u_blocks[q] = send_cols(u_low, q)
    for q in reversed(range(1, n_rows)):
        v_blocks[q] = send_rows(v_low, q)
    for q in [0] + far:
        u_blocks[q ^ 1] = send_cols(u_blocks[q], 1)

    sds = jax.ShapeDtypeStruct
    pairs = n_cols // 2
    same, cross, pv = vmem_call(
        functools.partial(tile_kernel, n_cols, n_rows, tile),
        (
            sds((pairs, block_rows, rank), bf16),
            sds((pairs, block_rows, rank), bf16),
            sds((n_rows, v_rows + LOSS_ROWS, rank), bf16),
        ),
        [pltpu.VMEM((n_rows * v_rows, rank), bf16), pltpu.VMEM((n_rows * v_rows, rank), f32)],
        1,
        5 + n_cols + n_rows,
        cost_estimate=pl.CostEstimate(
            flops=6 * slots * tile * tile * rank,
            bytes_accessed=2 * slots * tile * tile,
            transcendentals=0,
        ),
    )(
        column_ids,
        tile_values,
        words,
        own_u,
        own_v,
        *[u_blocks[q] for q in range(n_cols)],
        *[v_blocks[q] for q in range(n_rows)],
    )

    got = send_cols(cross, 1)
    v_got = [send_rows(pv[q], q) for q in range(1, n_rows)]
    sums = vmem_call(
        pair_kernel, tuple(sds((block_rows, rank), bf16) for _ in range(pairs)), (), 0, 2
    )(same, got)
    u_got = {q: send_cols(sums[q // 2], q) for q in far}
    new_v, loss = vmem_call(
        functools.partial(v_kernel, n_rows),
        (sds((v_rows, rank), f32), sds((8, rank), f32)),
        (),
        0,
        1 + n_rows,
    )(own_v, pv, *v_got)
    loss = loss + send_cols(loss, 1)
    loss_got = [send_cols(loss, q) for q in far]
    entries = n_rows * n_cols * slots * tile * tile
    new_u, loss = vmem_call(
        functools.partial(u_kernel, pairs, entries),
        (sds((block_rows, rank), f32), sds((8, rank), f32)),
        (),
        0,
        1 + 2 * pairs,
    )(own_u, sums[0], *[u_got[q] for q in far], loss, *loss_got)
    return new_u[None], new_v[None], loss[0, 0]


def solution(mesh):
    in_specs = (
        P("rows", "cols", None),
        P("cols", "rows", None),
        P("rows", "cols", None, None, None),
        P("rows", "cols", None, None, None),
        P("rows", "cols", None),
    )
    out_specs = (P("rows", "cols", None), P("cols", "rows", None), P())
    return jax.shard_map(
        per_device, mesh=mesh, in_specs=in_specs, out_specs=out_specs, check_vma=False
    )
```

```python
import functools

import jax
import jax.numpy as jnp
from jax import lax
from jax.experimental import pallas as pl
from jax.experimental.pallas import tpu as pltpu
from jax.sharding import PartitionSpec as P


step_rate = 0.01
ridge_weight = 0.1
bf16 = jnp.bfloat16
f32 = jnp.float32
LOSS_ROWS = 16
WORD_BITS = 16
VMEM_LIMIT = 24 * 2**20
sds = jax.ShapeDtypeStruct


def partners(size, bit):
    return [(i, i ^ bit) for i in range(size)]


def far_order(n_cols):
    return sorted(range(2, n_cols, 2), key=lambda q: (q != 4, -q))


def row_order(n_rows):
    return list(range(1, n_rows))


def call(body, out_shape, args, scratch=(), spaces=None, flops=0):
    spaces = spaces or {}
    specs = [pl.BlockSpec(memory_space=spaces.get(i, pltpu.VMEM)) for i in range(len(args))]
    return pl.pallas_call(
        body,
        out_shape=out_shape,
        in_specs=specs,
        out_specs=jax.tree.map(lambda _: pl.BlockSpec(memory_space=pltpu.VMEM), out_shape),
        scratch_shapes=list(scratch),
        compiler_params=pltpu.CompilerParams(vmem_limit_bytes=VMEM_LIMIT),
        cost_estimate=pl.CostEstimate(flops=flops, bytes_accessed=0, transcendentals=0),
    )(*args)


def pack_loss(loss_row):
    width = loss_row.shape[-1]
    hi = loss_row.astype(bf16).astype(f32)
    mid = (loss_row - hi).astype(bf16).astype(f32)
    lo = loss_row - hi - mid
    which = lax.broadcasted_iota(jnp.int32, (LOSS_ROWS, width), 0)
    rows = jnp.where(which == 0, hi, jnp.where(which == 1, mid, jnp.where(which == 2, lo, 0.0)))
    return rows.astype(bf16)


def read_loss(block):
    rows = block[...].astype(f32)
    return rows[0:1] + rows[1:2] + rows[2:3]


def fetch_kernel(*refs):
    count = len(refs) // 2
    sems = refs[-1]
    copies = [
        pltpu.make_async_copy(refs[i], refs[count + i], sems.at[i]) for i in range(count)
    ]
    for copy in copies:
        copy.start()
    for copy in copies:
        copy.wait()


def tile_kernel(n_cols, n_rows, tile, *refs):
    column_ids, values, words, own_u, own_v = refs[:5]
    u_blocks = refs[5 : 5 + n_cols]
    v_blocks = refs[5 + n_cols : 5 + n_cols + n_rows]
    low_out, v_band, *v_parts, v_total = refs[5 + n_cols + n_rows :]
    col = lax.axis_index("cols")
    row = lax.axis_index("rows")
    v_rows = own_v.shape[0]
    for q in range(n_rows):
        v_band[pl.ds((row ^ q) * v_rows, v_rows), :] = v_blocks[q][...]
    v_total[...] = jnp.zeros_like(v_total)
    block_rows = u_blocks[0].shape[0]
    bit = jnp.left_shift(1, lax.broadcasted_iota(jnp.int32, (WORD_BITS, tile), 0))
    squares = jnp.zeros((8, tile), f32)
    tiles = block_rows // tile
    for q in range(n_cols):
        for t in range(tiles):
            slot = (col ^ q) * tiles + t
            start = column_ids[slot] * tile
            left = u_blocks[q][t * tile : (t + 1) * tile, :]
            right = v_band[pl.ds(start, tile), :]
            predicted = lax.dot_general(
                left, right, (((1,), (1,)), ((), ())), preferred_element_type=f32
            )
            diff = predicted - values[slot].astype(f32)
            parts = []
            for w in range(tile // WORD_BITS):
                marks = jnp.broadcast_to(words[slot, w : w + 1, :], (WORD_BITS, tile))
                seen = jnp.bitwise_and(marks, bit) != 0
                parts.append(jnp.where(seen, diff[w * WORD_BITS : (w + 1) * WORD_BITS, :], 0.0))
            residual = jnp.concatenate(parts, axis=0)
            squares += jnp.sum((residual * residual).reshape(-1, 8, tile), axis=0)
            low = residual.astype(bf16)
            low_out[q * tiles + t] = low
            v_total[pl.ds(start, tile), :] += lax.dot_general(
                low, left, (((0,), (0,)), ((), ())), preferred_element_type=f32
            )
    u_own = own_u[...]
    v_own = own_v[...]
    loss = 0.5 * jnp.sum(squares) + 0.5 * ridge_weight * (
        jnp.sum(u_own * u_own) + jnp.sum(v_own * v_own)
    )
    packed = pack_loss(jnp.full((1, v_band.shape[-1]), loss, f32))
    for q in range(n_rows):
        v_parts[q][:v_rows, :] = v_total[pl.ds((row ^ q) * v_rows, v_rows), :].astype(bf16)
        v_parts[q][v_rows:, :] = packed


def rows_kernel(n_cols, tile, column_ids, low, v_band, same, cross):
    col = lax.axis_index("cols")
    tiles = low.shape[0] // n_cols
    for q in range(n_cols):
        target = cross if q & 1 else same
        for t in range(tiles):
            start = column_ids[(col ^ q) * tiles + t] * tile
            grad = jnp.dot(
                low[q * tiles + t], v_band[pl.ds(start, tile), :], preferred_element_type=f32
            )
            target[q // 2, t * tile : (t + 1) * tile, :] = grad.astype(bf16)


def v_sum_kernel(*refs):
    parts, (total_out, loss_out) = refs[:-2], refs[-2:]
    v_rows = total_out.shape[0]
    total = parts[0][:v_rows, :].astype(f32)
    loss = read_loss(parts[0].at[v_rows:])
    for part in parts[1:]:
        total += part[:v_rows, :].astype(f32)
        loss += read_loss(part.at[v_rows:])
    total_out[...] = total
    loss_out[...] = jnp.broadcast_to(loss, loss_out.shape)


def carry_kernel(loss, loss_other, same, got, *outs):
    total = loss[0:1] + loss_other[0:1]
    packed = pack_loss(total)
    rows = same.shape[1]
    for q, out in enumerate(outs):
        out[:rows, :] = (same[q].astype(f32) + got[q].astype(f32)).astype(bf16)
        out[rows:, :] = packed


def v_new_kernel(own_v, total, new_v):
    own = own_v[...]
    new_v[...] = own - step_rate * (total[...] + ridge_weight * own)


def u_new_kernel(entries, own_u, *refs):
    parts, (new_u, loss_out) = refs[:-2], refs[-2:]
    own = own_u[...]
    rows = own.shape[0]
    total = parts[0][:rows, :].astype(f32)
    loss = read_loss(parts[0].at[rows:])
    for part in parts[1:]:
        total += part[:rows, :].astype(f32)
        loss += read_loss(part.at[rows:])
    new_u[...] = own - step_rate * (total + ridge_weight * own)
    loss_out[...] = (loss * (1.0 / entries))[0:1, 0:1]


def per_device(factor_u, factor_v, values, mask_words, tile_cols):
    slots, tile = values.shape[2], values.shape[-1]
    rank = factor_u.shape[-1]
    n_rows, n_cols = lax.axis_size("rows"), lax.axis_size("cols")
    block_rows, v_rows = factor_u.shape[1], factor_v.shape[1]
    far = far_order(n_cols)
    pairs = n_cols // 2

    def send_cols(x, bit):
        return lax.ppermute(x, "cols", partners(n_cols, bit))

    def send_rows(x, bit):
        return lax.ppermute(x, "rows", partners(n_rows, bit))

    own_u, own_v = factor_u[0], factor_v[0]
    u_low, v_low = own_u.astype(bf16), own_v.astype(bf16)
    tile_values, words, column_ids = values[0, 0], mask_words[0, 0], tile_cols[0, 0]
    tile_values, words, column_ids = call(
        fetch_kernel,
        tuple(sds(x.shape, x.dtype) for x in (tile_values, words, column_ids)),
        (tile_values, words, column_ids),
        [pltpu.SemaphoreType.DMA((3,))],
        {i: pltpu.HBM for i in range(3)},
    )

    v_blocks = {0: v_low}
    for q in row_order(n_rows):
        v_blocks[q] = send_rows(v_low, q)
    u_blocks = {0: u_low}
    for q in far:
        u_blocks[q] = send_cols(u_low, q)
    for q in [0] + far:
        u_blocks[q ^ 1] = send_cols(u_blocks[q], 1)

    share = sds((v_rows + LOSS_ROWS, rank), bf16)
    low, v_band, *v_parts = call(
        functools.partial(tile_kernel, n_cols, n_rows, tile),
        (sds((slots, tile, tile), bf16), sds((n_rows * v_rows, rank), bf16)) + (share,) * n_rows,
        (
            column_ids,
            tile_values,
            words,
            own_u,
            own_v,
            *[u_blocks[q] for q in range(n_cols)],
            *[v_blocks[q] for q in range(n_rows)],
        ),
        [pltpu.VMEM((n_rows * v_rows, rank), f32)],
        {0: pltpu.SMEM},
        4 * slots * tile * tile * rank,
    )
    v_got = [send_rows(v_parts[q], q) for q in row_order(n_rows)]
    part = sds((pairs, block_rows, rank), bf16)
    same, cross = call(
        functools.partial(rows_kernel, n_cols, tile),
        (part, part),
        (column_ids, low, v_band),
        (),
        {0: pltpu.SMEM},
        2 * slots * tile * tile * rank,
    )
    got = send_cols(cross, 1)
    v_total, loss = call(
        v_sum_kernel, (sds((v_rows, rank), f32), sds((8, rank), f32)), (v_parts[0], *v_got)
    )
    loss_other = send_cols(loss, 1)
    wide = sds((block_rows + LOSS_ROWS, rank), bf16)
    sums = call(carry_kernel, (wide,) * pairs, (loss, loss_other, same, got))
    u_got = [send_cols(sums[q // 2], q) for q in far]
    new_v = call(v_new_kernel, sds((v_rows, rank), f32), (own_v, v_total))
    entries = n_rows * n_cols * slots * tile * tile
    new_u, loss = call(
        functools.partial(u_new_kernel, entries),
        (sds((block_rows, rank), f32), sds((1, 1), f32)),
        (own_u, sums[0], *u_got),
    )
    return new_u[None], new_v[None], loss.reshape(())


def solution(mesh):
    in_specs = (
        P("rows", "cols", None),
        P("cols", "rows", None),
        P("rows", "cols", None, None, None),
        P("rows", "cols", None, None, None),
        P("rows", "cols", None),
    )
    out_specs = (P("rows", "cols", None), P("cols", "rows", None), P())
    return jax.shard_map(
        per_device, mesh=mesh, in_specs=in_specs, out_specs=out_specs, check_vma=False
    )
```

```python
import functools

import jax
import jax.numpy as jnp
from jax import lax
from jax.experimental import pallas as pl
from jax.experimental.pallas import tpu as pltpu
from jax.sharding import PartitionSpec as P


step_rate = 0.01
ridge_weight = 0.1
bf16 = jnp.bfloat16
f32 = jnp.float32
LOSS_ROWS = 16
WORD_BITS = 16
PLAIN = 1
CROSS = 0
VMEM_LIMIT = 24 * 2**20
sds = jax.ShapeDtypeStruct


def partners(size, bit):
    return [(i, i ^ bit) for i in range(size)]


def bits_of(size):
    return [1 << i for i in range(size.bit_length() - 1)]


def far_order(n_cols):
    return [q ^ CROSS for q in sorted(range(2, n_cols, 2), key=lambda q: (q != 4, -q))]


def call(body, out_shape, args, scratch=(), spaces=None, flops=0):
    spaces = spaces or {}
    specs = [pl.BlockSpec(memory_space=spaces.get(i, pltpu.VMEM)) for i in range(len(args))]
    return pl.pallas_call(
        body,
        out_shape=out_shape,
        in_specs=specs,
        out_specs=jax.tree.map(lambda _: pl.BlockSpec(memory_space=pltpu.VMEM), out_shape),
        scratch_shapes=list(scratch),
        compiler_params=pltpu.CompilerParams(vmem_limit_bytes=VMEM_LIMIT),
        cost_estimate=pl.CostEstimate(flops=flops, bytes_accessed=0, transcendentals=0),
    )(*args)


def pack_loss(loss_row):
    width = loss_row.shape[-1]
    hi = loss_row.astype(bf16).astype(f32)
    mid = (loss_row - hi).astype(bf16).astype(f32)
    lo = loss_row - hi - mid
    which = lax.broadcasted_iota(jnp.int32, (LOSS_ROWS, width), 0)
    rows = jnp.where(which == 0, hi, jnp.where(which == 1, mid, jnp.where(which == 2, lo, 0.0)))
    return rows.astype(bf16)


def read_loss(block):
    rows = block[...].astype(f32)
    return rows[0:1] + rows[1:2] + rows[2:3]


def fetch_kernel(*refs):
    count = len(refs) // 2
    sems = refs[-1]
    copies = [
        pltpu.make_async_copy(refs[i], refs[count + i], sems.at[i]) for i in range(count)
    ]
    for copy in copies:
        copy.start()
    for copy in copies:
        copy.wait()


def stack_kernel(left, right, out):
    rows = left.shape[0]
    out[:rows, :] = left[...]
    out[rows:, :] = right[...]


def column_of(column_ids, slot):
    places = lax.broadcasted_iota(jnp.int32, column_ids.shape, 1)
    picked = jnp.where(places == slot, column_ids[...].astype(f32), 0.0)
    return jnp.sum(picked).astype(jnp.int32)


def tile_slots(places, tile, column_ids, values, words, u_blocks, v_band, low_out, right_out, v_total):
    col = lax.axis_index("cols")
    bit = jnp.left_shift(1, lax.broadcasted_iota(jnp.int32, (WORD_BITS, tile), 0))
    squares = jnp.zeros((8, tile), f32)
    tiles = u_blocks[0].shape[0] // tile
    for k, q in enumerate(places):
        for t in range(tiles):
            slot = (col ^ q) * tiles + t
            start = column_of(column_ids, slot) * tile
            left = u_blocks[k][t * tile : (t + 1) * tile, :]
            right = v_band[pl.ds(start, tile), :]
            predicted = lax.dot_general(
                left, right, (((1,), (1,)), ((), ())), preferred_element_type=f32
            )
            diff = predicted - values[slot].astype(f32)
            parts = []
            for w in range(tile // WORD_BITS):
                marks = jnp.broadcast_to(words[slot, w : w + 1, :], (WORD_BITS, tile))
                seen = jnp.bitwise_and(marks, bit) != 0
                parts.append(jnp.where(seen, diff[w * WORD_BITS : (w + 1) * WORD_BITS, :], 0.0))
            residual = jnp.concatenate(parts, axis=0)
            squares += jnp.sum((residual * residual).reshape(-1, 8, tile), axis=0)
            low = residual.astype(bf16)
            low_out[k * tiles + t] = low
            right_out[k * tiles + t] = right
            v_total[pl.ds(start, tile), :] += lax.dot_general(
                low, left, (((0,), (0,)), ((), ())), preferred_element_type=f32
            )
    return squares


def even_kernel(places, order_v, tile, *refs):
    column_ids, values, words = refs[:3]
    u_blocks, (v_stack, v_other, low_out, right_out, v_band, v_total, squares) = (
        refs[3:-7],
        refs[-7:],
    )
    row = lax.axis_index("rows")
    n_rows = len(order_v)
    v_rows = v_band.shape[0] // n_rows
    half = n_rows // 2
    for k, q in enumerate(order_v):
        source = v_stack if k < half else v_other
        v_band[pl.ds((row ^ q) * v_rows, v_rows), :] = source[
            (k % half) * v_rows : (k % half + 1) * v_rows, :
        ]
    v_total[...] = jnp.zeros_like(v_total)
    squares[...] = tile_slots(
        places, tile, column_ids, values, words, u_blocks, v_band, low_out, right_out, v_total
    )


def odd_kernel(places, n_rows, tile, *refs):
    column_ids, values, words, own_u, own_v, v_band, v_start, squares = refs[:8]
    u_blocks, (low_out, right_out, keep, send, loss_out, v_total) = refs[8:-6], refs[-6:]
    row = lax.axis_index("rows")
    v_total[...] = v_start[...]
    total = squares[...] + tile_slots(
        places, tile, column_ids, values, words, u_blocks, v_band, low_out, right_out, v_total
    )
    u_own = own_u[...]
    v_own = own_v[...]
    loss = 0.5 * jnp.sum(total) + 0.5 * ridge_weight * (
        jnp.sum(u_own * u_own) + jnp.sum(v_own * v_own)
    )
    loss_out[...] = jnp.full(loss_out.shape, loss, f32)
    v_rows = own_v.shape[0]
    keep[...] = v_total[pl.ds(row * v_rows, v_rows), :]
    for q in range(1, n_rows):
        send[q - 1] = v_total[pl.ds((row ^ q) * v_rows, v_rows), :].astype(bf16)


def rows_kernel(low_even, low_odd, right_even, right_odd, same, cross):
    pairs, tile = same.shape[0], low_even.shape[1]
    tiles = low_even.shape[0] // pairs
    for low, right, target in ((low_odd, right_odd, cross), (low_even, right_even, same)):
        for k in range(pairs):
            for t in range(tiles):
                slot = k * tiles + t
                grad = jnp.dot(low[slot], right[slot], preferred_element_type=f32)
                target[k, t * tile : (t + 1) * tile, :] = grad.astype(bf16)


def pack_kernel(loss, loss_other, blocks, *outs):
    total = loss[...] + loss_other[...]
    packed = pack_loss(total[0:1])
    rows = blocks.shape[1]
    for q, out in enumerate(outs[:-1]):
        out[:rows, :] = blocks[q]
        out[rows:, :] = packed
    outs[-1][...] = total


def carry_kernel(count, loss, *refs):
    blocks, outs = refs[:count], refs[count:]
    packed = pack_loss(loss[0:1])
    for block, out in zip(blocks, outs):
        rows = block.shape[0]
        out[:rows, :] = block[...]
        out[rows:, :] = packed


def pair_kernel(same, got, *outs):
    for q, out in enumerate(outs):
        out[...] = (same[q].astype(f32) + got[q].astype(f32)).astype(bf16)


def fold_kernel(keep, loss, *refs):
    parts, (total_out, loss_out) = refs[:-2], refs[-2:]
    rows = keep.shape[0]
    total, loss_sum = keep[...], loss[...]
    for part in parts:
        total += part[:rows, :].astype(f32)
        loss_sum += read_loss(part.at[rows:])
    total_out[...] = total
    loss_out[...] = loss_sum


def v_new_kernel(own_v, total, new_v):
    own = own_v[...]
    new_v[...] = own - step_rate * (total[...] + ridge_weight * own)


def u_new_kernel(entries, n_tiny, own_u, loss, *refs):
    tiny, parts, (new_u, loss_out) = refs[:n_tiny], refs[n_tiny:-2], refs[-2:]
    own = own_u[...]
    rows = own.shape[0]
    total = parts[0][:rows, :].astype(f32)
    for part in parts[1:]:
        total += part[:rows, :].astype(f32)
    loss_sum = loss[0:1]
    for part in parts[1 + n_tiny :]:
        loss_sum += read_loss(part.at[rows:])
    for other in tiny:
        loss_sum += other[0:1]
    new_u[...] = own - step_rate * (total + ridge_weight * own)
    loss_out[...] = (loss_sum * (1.0 / entries))[0:1, 0:1]


def per_device(factor_u, factor_v, values, mask_words, tile_cols):
    slots, tile = values.shape[2], values.shape[-1]
    rank = factor_u.shape[-1]
    n_rows, n_cols = lax.axis_size("rows"), lax.axis_size("cols")
    block_rows, v_rows = factor_u.shape[1], factor_v.shape[1]
    far = far_order(n_cols)
    direct = [0] + far
    swapped = [q ^ 1 for q in direct]
    pairs = n_cols // 2
    row_bits = bits_of(n_rows)

    def send_cols(x, bit):
        return lax.ppermute(x, "cols", partners(n_cols, bit))

    def send_rows(x, bit):
        return lax.ppermute(x, "rows", partners(n_rows, bit))

    own_u, own_v = factor_u[0], factor_v[0]
    u_low, v_low = own_u.astype(bf16), own_v.astype(bf16)
    held = (values[0, 0], mask_words[0, 0], tile_cols[0, 0])
    tile_values, words, column_ids = call(
        fetch_kernel,
        tuple(sds(x.shape, x.dtype) for x in held),
        tuple(pltpu.with_memory_space_constraint(x, pltpu.HBM) for x in held),
        [pltpu.SemaphoreType.DMA((len(held),))],
        {i: pltpu.HBM for i in range(len(held))},
    )
    column_ids = column_ids.reshape(1, slots)

    v_stack, order_v = v_low, [0]
    for b in row_bits:
        v_other = send_rows(v_stack, b)
        order_v = order_v + [q ^ b for q in order_v]
        if b != row_bits[-1]:
            shape = sds((2 * v_stack.shape[0], rank), bf16)
            v_stack = call(stack_kernel, shape, (v_stack, v_other))
    u_blocks = {0: u_low}
    for q in far:
        u_blocks[q] = send_cols(u_low, q)
    for q in direct:
        u_blocks[q ^ 1] = send_cols(u_blocks[q], 1)

    low_shape = sds((slots // 2, tile, tile), bf16)
    right_shape = sds((slots // 2, tile, rank), bf16)
    band = (n_rows * v_rows, rank)
    tile_flops = 2 * slots * tile * tile * rank
    low_even, right_even, v_band, v_start, squares = call(
        functools.partial(even_kernel, direct, order_v, tile),
        (low_shape, right_shape, sds(band, bf16), sds(band, f32), sds((8, tile), f32)),
        (
            column_ids,
            tile_values,
            words,
            *[u_blocks[q] for q in direct],
            v_stack,
            v_other,
        ),
        flops=tile_flops,
    )
    low_odd, right_odd, keep, send, loss = call(
        functools.partial(odd_kernel, swapped, n_rows, tile),
        (
            low_shape,
            right_shape,
            sds((v_rows, rank), f32),
            sds((n_rows - 1, v_rows, rank), bf16),
            sds((8, rank), f32),
        ),
        (
            column_ids,
            tile_values,
            words,
            own_u,
            own_v,
            v_band,
            v_start,
            squares,
            *[u_blocks[q] for q in swapped],
        ),
        [pltpu.VMEM(band, f32)],
        flops=tile_flops,
    )
    loss_other = send_cols(loss, 1)
    part = sds((pairs, block_rows, rank), bf16)
    same, cross = call(
        rows_kernel, (part, part), (low_even, low_odd, right_even, right_odd), flops=tile_flops
    )
    got = send_cols(cross, 1)
    loss_shape = sds((8, rank), f32)
    share = sds((v_rows + LOSS_ROWS, rank), bf16)
    *shares, loss = call(
        pack_kernel, (share,) * (n_rows - 1) + (loss_shape,), (loss, loss_other, send)
    )
    block = sds((block_rows, rank), bf16)
    sums = call(pair_kernel, (block,) * pairs, (same, got))
    plain, carrying = far[:PLAIN], far[PLAIN:]
    u_got = [send_cols(sums[direct.index(q)], q) for q in plain]
    v_got = [send_rows(x, q) for q, x in enumerate(shares, 1)]
    keep, loss = call(fold_kernel, (sds((v_rows, rank), f32), loss_shape), (keep, loss, *v_got))
    wide = sds((block_rows + LOSS_ROWS, rank), bf16)
    carried = call(
        functools.partial(carry_kernel, len(carrying)),
        (wide,) * len(carrying),
        (loss, *[sums[direct.index(q)] for q in carrying]),
    )
    u_got += [send_cols(x, q) for q, x in zip(carrying, carried)]
    tiny = [send_cols(loss, q) for q in plain]
    new_v = call(v_new_kernel, sds((v_rows, rank), f32), (own_v, keep))
    entries = n_rows * n_cols * slots * tile * tile
    new_u, loss = call(
        functools.partial(u_new_kernel, entries, len(tiny)),
        (sds((block_rows, rank), f32), sds((1, 1), f32)),
        (own_u, loss, *tiny, sums[0], *u_got),
    )
    return new_u[None], new_v[None], loss.reshape(())


def solution(mesh):
    in_specs = (
        P("rows", "cols", None),
        P("cols", "rows", None),
        P("rows", "cols", None, None, None),
        P("rows", "cols", None, None, None),
        P("rows", "cols", None),
    )
    out_specs = (P("rows", "cols", None), P("cols", "rows", None), P())
    return jax.shard_map(
        per_device, mesh=mesh, in_specs=in_specs, out_specs=out_specs, check_vma=False
    )
```

```python
import functools

import jax
import jax.numpy as jnp
from jax import lax
from jax.experimental import pallas as pl
from jax.experimental.pallas import tpu as pltpu
from jax.sharding import PartitionSpec as P


step_rate = 0.01
ridge_weight = 0.1
bf16 = jnp.bfloat16
f32 = jnp.float32
LOSS_ROWS = 16
WORD_BITS = 16
PLAIN = 1
VMEM_LIMIT = 24 * 2**20
sds = jax.ShapeDtypeStruct


def partners(size, bit):
    return [(i, i ^ bit) for i in range(size)]


def bits_of(size):
    return [1 << i for i in range(size.bit_length() - 1)]


def far_order(n_cols):
    return sorted(range(2, n_cols, 2), key=lambda q: (q != 4, -q))


def call(body, out_shape, args, scratch=(), spaces=None, flops=0):
    spaces = spaces or {}
    specs = [pl.BlockSpec(memory_space=spaces.get(i, pltpu.VMEM)) for i in range(len(args))]
    return pl.pallas_call(
        body,
        out_shape=out_shape,
        in_specs=specs,
        out_specs=jax.tree.map(lambda _: pl.BlockSpec(memory_space=pltpu.VMEM), out_shape),
        scratch_shapes=list(scratch),
        compiler_params=pltpu.CompilerParams(vmem_limit_bytes=VMEM_LIMIT),
        cost_estimate=pl.CostEstimate(flops=flops, bytes_accessed=0, transcendentals=0),
    )(*args)


def pack_loss(loss_row):
    width = loss_row.shape[-1]
    hi = loss_row.astype(bf16).astype(f32)
    mid = (loss_row - hi).astype(bf16).astype(f32)
    lo = loss_row - hi - mid
    which = lax.broadcasted_iota(jnp.int32, (LOSS_ROWS, width), 0)
    rows = jnp.where(which == 0, hi, jnp.where(which == 1, mid, jnp.where(which == 2, lo, 0.0)))
    return rows.astype(bf16)


def read_loss(block):
    rows = block[...].astype(f32)
    return rows[0:1] + rows[1:2] + rows[2:3]


def low_kernel(u_hbm, v_hbm, u_own, v_own, u_low, v_low, sems):
    rows = u_hbm.shape[0] // 2
    copies = [
        pltpu.make_async_copy(u_hbm.at[:rows], u_own.at[:rows], sems.at[0]),
        pltpu.make_async_copy(u_hbm.at[rows:], u_own.at[rows:], sems.at[1]),
        pltpu.make_async_copy(v_hbm, v_own, sems.at[2]),
    ]
    for copy in copies:
        copy.start()
    copies[0].wait()
    u_low[:rows, :] = u_own[:rows, :].astype(bf16)
    copies[1].wait()
    u_low[rows:, :] = u_own[rows:, :].astype(bf16)
    copies[2].wait()
    v_low[...] = v_own[...].astype(bf16)


def decode_kernel(values_hbm, words_hbm, ids_hbm, seen, marked, ids, values, words, sems):
    slots, tile = values.shape[0], values.shape[1]
    copies = [
        pltpu.make_async_copy(words_hbm, words, sems.at[slots]),
        pltpu.make_async_copy(ids_hbm, ids, sems.at[slots + 1]),
    ]
    copies += [
        pltpu.make_async_copy(values_hbm.at[s], values.at[s], sems.at[s]) for s in range(slots)
    ]
    for copy in copies:
        copy.start()
    copies[0].wait()
    bit = jnp.left_shift(1, lax.broadcasted_iota(jnp.int32, (WORD_BITS, tile), 0))
    for s in range(slots):
        copies[2 + s].wait()
        for w in range(tile // WORD_BITS):
            rows = slice(w * WORD_BITS, (w + 1) * WORD_BITS)
            marks = jnp.broadcast_to(words[s, w : w + 1, :], (WORD_BITS, tile))
            hit = jnp.bitwise_and(marks, bit) != 0
            seen[s, rows, :] = jnp.where(hit, 1.0, 0.0)
            marked[s, rows, :] = jnp.where(hit, values[s, rows, :].astype(f32), 0.0)
    copies[1].wait()


def stack_kernel(left, right, out):
    rows = left.shape[0]
    out[:rows, :] = left[...]
    out[rows:, :] = right[...]


def column_starts(places, tiles, tile, column_ids):
    col = lax.axis_index("cols")
    ids = column_ids[...].astype(f32)
    lanes = lax.broadcasted_iota(jnp.int32, ids.shape, 1)
    slots = [(col ^ q) * tiles + t for q in places for t in range(tiles)]
    picked = [jnp.sum(jnp.where(lanes == slot, ids, 0.0)) for slot in slots]
    return slots, [x.astype(jnp.int32) * tile for x in picked]


def residuals(slots, seen, marked, u_blocks, right, low_out):
    tile = low_out.shape[-1]
    tiles = u_blocks[0].shape[0] // tile
    squares = jnp.zeros((8, tile), f32)
    for k, slot in enumerate(slots):
        t = k % tiles
        predicted = lax.dot_general(
            u_blocks[k // tiles][t * tile : (t + 1) * tile, :],
            right[k],
            (((1,), (1,)), ((), ())),
            preferred_element_type=f32,
        )
        residual = seen[slot] * predicted - marked[slot]
        squares += jnp.sum((residual * residual).reshape(-1, 8, tile), axis=0)
        low_out[k] = residual.astype(bf16)
    return squares


def column_grads(starts, low, u_blocks, v_total):
    tile = low.shape[-1]
    tiles = u_blocks[0].shape[0] // tile
    for k, start in enumerate(starts):
        t = k % tiles
        v_total[pl.ds(start, tile), :] += lax.dot_general(
            low[k],
            u_blocks[k // tiles][t * tile : (t + 1) * tile, :],
            (((0,), (0,)), ((), ())),
            preferred_element_type=f32,
        )


def even_kernel(direct, swapped, order_v, tile, *refs):
    column_ids, seen, marked = refs[:3]
    u_blocks, (v_stack, v_other, low, right, right_odd, v_total, squares, v_band) = (
        refs[3:-8],
        refs[-8:],
    )
    tiles = u_blocks[0].shape[0] // tile
    slots, starts = column_starts(direct, tiles, tile, column_ids)
    _, starts_odd = column_starts(swapped, tiles, tile, column_ids)
    row = lax.axis_index("rows")
    n_rows = len(order_v)
    v_rows = v_band.shape[0] // n_rows
    half = n_rows // 2
    for k, q in enumerate(order_v):
        source = v_stack if k < half else v_other
        v_band[pl.ds((row ^ q) * v_rows, v_rows), :] = source[
            (k % half) * v_rows : (k % half + 1) * v_rows, :
        ]
    v_total[...] = jnp.zeros_like(v_total)
    for out, places in ((right, starts), (right_odd, starts_odd)):
        for k, start in enumerate(places):
            out[k] = v_band[pl.ds(start, tile), :]
    squares[...] = residuals(slots, seen, marked, u_blocks, right, low)
    column_grads(starts, low, u_blocks, v_total)


def odd_kernel(swapped, tile, *refs):
    seen, marked, own_u, own_v, right, squares = refs[:6]
    u_blocks, (low, loss_out) = refs[6:-2], refs[-2:]
    col = lax.axis_index("cols")
    tiles = u_blocks[0].shape[0] // tile
    slots = [(col ^ q) * tiles + t for q in swapped for t in range(tiles)]
    total = squares[...] + residuals(slots, seen, marked, u_blocks, right, low)
    u_own = own_u[...]
    v_own = own_v[...]
    loss = 0.5 * jnp.sum(total) + 0.5 * ridge_weight * (
        jnp.sum(u_own * u_own) + jnp.sum(v_own * v_own)
    )
    loss_out[...] = jnp.full(loss_out.shape, loss, f32)


def rows_kernel(low, right, cross):
    pairs, tile = cross.shape[0], low.shape[1]
    tiles = low.shape[0] // pairs
    for k in range(pairs):
        for t in range(tiles):
            grad = jnp.dot(low[k * tiles + t], right[k * tiles + t], preferred_element_type=f32)
            cross[k, t * tile : (t + 1) * tile, :] = grad.astype(bf16)


def columns_kernel(swapped, tile, *refs):
    column_ids, low, v_start = refs[:3]
    u_blocks, (keep, send, v_total) = refs[3:-3], refs[-3:]
    row = lax.axis_index("rows")
    _, starts = column_starts(swapped, u_blocks[0].shape[0] // tile, tile, column_ids)
    v_total[...] = v_start[...]
    column_grads(starts, low, u_blocks, v_total)
    v_rows = keep.shape[0]
    keep[...] = v_total[pl.ds(row * v_rows, v_rows), :]
    for q in range(1, send.shape[0] + 1):
        send[q - 1] = v_total[pl.ds((row ^ q) * v_rows, v_rows), :].astype(bf16)


def pack_kernel(loss, loss_other, blocks, *outs):
    total = loss[...] + loss_other[...]
    packed = pack_loss(total[0:1])
    rows = blocks.shape[1]
    for q, out in enumerate(outs[:-1]):
        out[:rows, :] = blocks[q]
        out[rows:, :] = packed
    outs[-1][...] = total


def carry_kernel(count, loss, *refs):
    blocks, outs = refs[:count], refs[count:]
    packed = pack_loss(loss[0:1])
    for block, out in zip(blocks, outs):
        rows = block.shape[0]
        out[:rows, :] = block[...]
        out[rows:, :] = packed


def pair_kernel(places, low, right, got, *outs):
    tile = low.shape[1]
    tiles = low.shape[0] // got.shape[0]
    for k, out in zip(places, outs):
        for t in range(tiles):
            rows = slice(t * tile, (t + 1) * tile)
            grad = jnp.dot(low[k * tiles + t], right[k * tiles + t], preferred_element_type=f32)
            out[rows, :] = (grad + got[k, rows, :].astype(f32)).astype(bf16)


def fold_kernel(keep, loss, *refs):
    parts, (total_out, loss_out) = refs[:-2], refs[-2:]
    rows = keep.shape[0]
    total, loss_sum = keep[...], loss[...]
    for part in parts:
        total += part[:rows, :].astype(f32)
        loss_sum += read_loss(part.at[rows:])
    total_out[...] = total
    loss_out[...] = loss_sum


def v_new_kernel(own_v, total, new_v):
    own = own_v[...]
    new_v[...] = own - step_rate * (total[...] + ridge_weight * own)


def u_new_kernel(entries, n_tiny, own_u, loss, *refs):
    tiny, parts, (new_u, loss_out) = refs[:n_tiny], refs[n_tiny:-2], refs[-2:]
    own = own_u[...]
    rows = own.shape[0]
    total = parts[0][:rows, :].astype(f32)
    for part in parts[1:]:
        total += part[:rows, :].astype(f32)
    loss_sum = loss[0:1]
    for part in parts[1 + n_tiny :]:
        loss_sum += read_loss(part.at[rows:])
    for other in tiny:
        loss_sum += other[0:1]
    new_u[...] = own - step_rate * (total + ridge_weight * own)
    loss_out[...] = (loss_sum * (1.0 / entries))[0:1, 0:1]


def per_device(factor_u, factor_v, values, mask_words, tile_cols):
    slots, tile = values.shape[2], values.shape[-1]
    rank = factor_u.shape[-1]
    n_rows, n_cols = lax.axis_size("rows"), lax.axis_size("cols")
    block_rows, v_rows = factor_u.shape[1], factor_v.shape[1]
    far = far_order(n_cols)
    direct = [0] + far
    swapped = [q ^ 1 for q in direct]
    pairs = n_cols // 2
    row_bits = bits_of(n_rows)

    def send_cols(x, bit):
        return lax.ppermute(x, "cols", partners(n_cols, bit))

    def send_rows(x, bit):
        return lax.ppermute(x, "rows", partners(n_rows, bit))

    block_f32, own_f32 = sds((block_rows, rank), f32), sds((v_rows, rank), f32)
    own_u, own_v, u_low, v_low = call(
        low_kernel,
        (block_f32, own_f32, sds((block_rows, rank), bf16), sds((v_rows, rank), bf16)),
        tuple(pltpu.with_memory_space_constraint(x[0], pltpu.HBM) for x in (factor_u, factor_v)),
        [pltpu.SemaphoreType.DMA((3,))],
        {0: pltpu.HBM, 1: pltpu.HBM},
    )
    held = (values[0, 0], mask_words[0, 0], tile_cols[0, 0])
    full = sds((slots, tile, tile), f32)
    seen, marked, column_ids = call(
        decode_kernel,
        (full, full, sds(held[2].shape, jnp.int32)),
        tuple(pltpu.with_memory_space_constraint(x, pltpu.HBM) for x in held),
        [
            pltpu.VMEM(held[0].shape, held[0].dtype),
            pltpu.VMEM(held[1].shape, held[1].dtype),
            pltpu.SemaphoreType.DMA((slots + 2,)),
        ],
        {i: pltpu.HBM for i in range(len(held))},
    )
    column_ids = column_ids.reshape(1, slots)

    v_stack, order_v = v_low, [0]
    for b in row_bits:
        v_other = send_rows(v_stack, b)
        order_v = order_v + [q ^ b for q in order_v]
        if b != row_bits[-1]:
            shape = sds((2 * v_stack.shape[0], rank), bf16)
            v_stack = call(stack_kernel, shape, (v_stack, v_other))
    u_blocks = {0: u_low}
    for q in far:
        u_blocks[q] = send_cols(u_low, q)
    for q in direct:
        u_blocks[q ^ 1] = send_cols(u_blocks[q], 1)

    low_shape = sds((slots // 2, tile, tile), bf16)
    right_shape = sds((slots // 2, tile, rank), bf16)
    band = (n_rows * v_rows, rank)
    tile_flops = 2 * slots * tile * tile * rank
    part = sds((pairs, block_rows, rank), bf16)
    low_even, right_even, right_odd, v_start, squares = call(
        functools.partial(even_kernel, direct, swapped, order_v, tile),
        (low_shape, right_shape, right_shape, sds(band, f32), sds((8, tile), f32)),
        (
            column_ids,
            seen,
            marked,
            *[u_blocks[q] for q in direct],
            v_stack,
            v_other,
        ),
        [pltpu.VMEM(band, bf16)],
        flops=tile_flops,
    )
    low_odd, loss = call(
        functools.partial(odd_kernel, swapped, tile),
        (low_shape, sds((8, rank), f32)),
        (
            seen,
            marked,
            own_u,
            own_v,
            right_odd,
            squares,
            *[u_blocks[q] for q in swapped],
        ),
        flops=tile_flops,
    )
    loss_other = send_cols(loss, 1)
    cross = call(rows_kernel, part, (low_odd, right_odd), flops=tile_flops)
    got = send_cols(cross, 1)
    keep, send = call(
        functools.partial(columns_kernel, swapped, tile),
        (sds((v_rows, rank), f32), sds((n_rows - 1, v_rows, rank), bf16)),
        (column_ids, low_odd, v_start, *[u_blocks[q] for q in swapped]),
        [pltpu.VMEM(band, f32)],
        flops=tile_flops,
    )
    loss_shape = sds((8, rank), f32)
    share = sds((v_rows + LOSS_ROWS, rank), bf16)
    *shares, loss = call(
        pack_kernel, (share,) * (n_rows - 1) + (loss_shape,), (loss, loss_other, send)
    )
    block = sds((block_rows, rank), bf16)
    first = list(range(1, 1 + PLAIN))
    rest = [0] + list(range(1 + PLAIN, pairs))
    sums = {}
    for places in (first, rest):
        outs = call(
            functools.partial(pair_kernel, places),
            (block,) * len(places),
            (low_even, right_even, got),
            flops=tile_flops // pairs,
        )
        sums.update(zip(places, outs))
    plain, carrying = far[:PLAIN], far[PLAIN:]
    u_got = [send_cols(sums[direct.index(q)], q) for q in plain]
    v_got = [send_rows(x, q) for q, x in enumerate(shares, 1)]
    keep, loss = call(fold_kernel, (sds((v_rows, rank), f32), loss_shape), (keep, loss, *v_got))
    wide = sds((block_rows + LOSS_ROWS, rank), bf16)
    carried = call(
        functools.partial(carry_kernel, len(carrying)),
        (wide,) * len(carrying),
        (loss, *[sums[direct.index(q)] for q in carrying]),
    )
    u_got += [send_cols(x, q) for q, x in zip(carrying, carried)]
    tiny = [send_cols(loss, q) for q in plain]
    new_v = call(v_new_kernel, sds((v_rows, rank), f32), (own_v, keep))
    entries = n_rows * n_cols * slots * tile * tile
    new_u, loss = call(
        functools.partial(u_new_kernel, entries, len(tiny)),
        (sds((block_rows, rank), f32), sds((1, 1), f32)),
        (own_u, loss, *tiny, sums[0], *u_got),
    )
    return new_u[None], new_v[None], loss.reshape(())


def solution(mesh):
    in_specs = (
        P("rows", "cols", None),
        P("cols", "rows", None),
        P("rows", "cols", None, None, None),
        P("rows", "cols", None, None, None),
        P("rows", "cols", None),
    )
    out_specs = (P("rows", "cols", None), P("cols", "rows", None), P())
    return jax.shard_map(
        per_device, mesh=mesh, in_specs=in_specs, out_specs=out_specs, check_vma=False
    )
```
